128 devices in a mesh: batch: 1, seq: 128 (over z, y, x, core).
Axes of the slice: x: 4, y: 4, z: 4, core: 2. Of those that a mesh axis runs over, the one named last changes fastest.
Arguments:
- tokens: bfloat16 [131072, 1536], P(('batch', 'seq'))
- w_query: bfloat16 [1536, 1536], replicated
- w_key: bfloat16 [1536, 1536], replicated
- w_value: bfloat16 [1536, 1536], replicated
- w_out: bfloat16 [1536, 1536], replicated
- selected: int32 [12, 1024, 16], P(None, ('batch', 'seq'))
Outputs:
- output: bfloat16 [131072, 1536], P(('batch', 'seq'))
All inputs are finite; a program needn't handle non-finite values.
Results may differ from the reference program's by a relative error of at most 0.00329631.
Values are sent between devices in bfloat16 or wider.
A program may use at most 1 GiB of HBM per device.

```python
import jax
import jax.numpy as jnp
from jax import lax

D_MODEL = 1536
NUM_HEADS = 12
HEAD_DIM = 128
BLOCK_SIZE = 128
RAND_BLOCKS = 16
BLOCKS_DEV = 8
SHARDS = 128
GLOBAL_BLOCKS = 2

NUM_BLOCKS = BLOCKS_DEV * SHARDS
SEQ_LEN = NUM_BLOCKS * BLOCK_SIZE
WIDTH = NUM_HEADS * HEAD_DIM


def draw_selection(rand_key):
    per_dev = BLOCKS_DEV * RAND_BLOCKS
    key_order, key_local = jax.random.split(rand_key)
    order_score = jax.random.randint(key_order, (NUM_HEADS, SHARDS, per_dev), 0, 2 ** 18) * per_dev + jnp.arange(per_dev, dtype=jnp.int32)
    slot_order = jnp.argsort(order_score, axis=-1)
    owner_dev = (jnp.arange(SHARDS, dtype=jnp.int32)[None, :, None] + slot_order % SHARDS) % SHARDS
    local_blk = jax.random.randint(key_local, (NUM_HEADS, SHARDS, per_dev), 0, BLOCKS_DEV)
    blocks = owner_dev * BLOCKS_DEV + local_blk
    return blocks.reshape(NUM_HEADS, NUM_BLOCKS, RAND_BLOCKS).astype(jnp.int32)


def setup_inputs(seed: int = 0, part: int = 0) -> dict:
    root_key = jax.random.key(seed)
    w_keys = jax.random.split(root_key, 4)
    part_key = jax.random.fold_in(jax.random.fold_in(root_key, 1000), part)
    key_tokens, key_select = jax.random.split(part_key)
    tokens = jax.random.normal(key_tokens, (SEQ_LEN, D_MODEL), jnp.float32).astype(jnp.bfloat16)
    in_scale = D_MODEL ** -0.5
    out_scale = ((RAND_BLOCKS + 5) * BLOCK_SIZE / (3.0 * WIDTH)) ** 0.5
    w_query = (jax.random.normal(w_keys[0], (D_MODEL, WIDTH), jnp.float32) * in_scale).astype(jnp.bfloat16)
    w_key = (jax.random.normal(w_keys[1], (D_MODEL, WIDTH), jnp.float32) * in_scale).astype(jnp.bfloat16)
    w_value = (jax.random.normal(w_keys[2], (D_MODEL, WIDTH), jnp.float32) * in_scale).astype(jnp.bfloat16)
    w_out = (jax.random.normal(w_keys[3], (D_MODEL, WIDTH), jnp.float32) * out_scale).astype(jnp.bfloat16)
    return {'tokens': tokens, 'w_query': w_query, 'w_key': w_key, 'w_value': w_value, 'w_out': w_out, 'selected': draw_selection(key_select)}


def pick_blocks(table_arr, row_index):
    return table_arr[row_index]


def reference(tokens, w_query, w_key, w_value, w_out, selected):
    score_scale = HEAD_DIM ** -0.5

    def project(weight):
        product = jnp.dot(tokens, weight, preferred_element_type=jnp.float32).astype(jnp.bfloat16)
        return product.reshape(NUM_BLOCKS, BLOCK_SIZE, NUM_HEADS, HEAD_DIM).transpose(2, 0, 1, 3)

    q_all = project(w_query)
    k_all = project(w_key)
    v_all = project(w_value)
    earlier = jnp.arange(RAND_BLOCKS)[None, :] < jnp.arange(RAND_BLOCKS)[:, None]
    offsets = jnp.arange(-1, 2)

    def ordinary(row_id):
        sel_ids = selected[:, row_id, :]
        window_raw = row_id + offsets
        window_ids = jnp.clip(window_raw, 0, NUM_BLOCKS - 1)
        fixed_ids = jnp.concatenate([jnp.arange(GLOBAL_BLOCKS), window_ids])
        all_ids = jnp.concatenate([jnp.broadcast_to(fixed_ids, (NUM_HEADS, GLOBAL_BLOCKS + 3)), sel_ids], axis=1)
        key_rows = jax.vmap(pick_blocks)(k_all, all_ids).astype(jnp.float32)
        val_rows = jax.vmap(pick_blocks)(v_all, all_ids).astype(jnp.float32)
        window_ok = (window_raw >= GLOBAL_BLOCKS) & (window_raw < NUM_BLOCKS)
        fixed_ok = jnp.concatenate([jnp.full((GLOBAL_BLOCKS,), True), window_ok])
        repeat = jnp.any((sel_ids[:, :, None] == sel_ids[:, None, :]) & earlier, axis=2)
        sel_ok = (sel_ids >= GLOBAL_BLOCKS) & (jnp.abs(sel_ids - row_id) > 1) & jnp.logical_not(repeat)
        key_ok = jnp.concatenate([jnp.broadcast_to(fixed_ok, (NUM_HEADS, GLOBAL_BLOCKS + 3)), sel_ok], axis=1)
        q_rows = q_all[:, row_id].astype(jnp.float32)
        scores = jnp.einsum('hqe,hkce->hqkc', q_rows, key_rows) * score_scale
        scores = jnp.where(key_ok[:, None, :, None], scores, -jnp.inf)
        row_max = jnp.max(scores, axis=(2, 3), keepdims=True)
        exp_scores = jnp.exp(scores - row_max)
        row_sum = jnp.sum(exp_scores, axis=(2, 3))
        row_acc = jnp.einsum('hqkc,hkce->hqe', exp_scores.astype(jnp.bfloat16).astype(jnp.float32), val_rows)
        return row_acc / row_sum[..., None]

    ordinary_out = lax.map(ordinary, jnp.arange(GLOBAL_BLOCKS, NUM_BLOCKS))

    glob_rows = GLOBAL_BLOCKS * BLOCK_SIZE
    glob_q = q_all[:, :GLOBAL_BLOCKS].reshape(NUM_HEADS, glob_rows, HEAD_DIM).astype(jnp.float32)

    def block_scores(key_blk):
        return jnp.einsum('hqe,hce->hqc', glob_q, k_all[:, key_blk].astype(jnp.float32)) * score_scale

    def block_max(key_blk):
        return jnp.max(block_scores(key_blk), axis=2)

    glob_max = jnp.max(lax.map(block_max, jnp.arange(NUM_BLOCKS)), axis=0)

    def accumulate(acc_state, key_blk):
        row_sum, row_acc = acc_state
        exp_scores = jnp.exp(block_scores(key_blk) - glob_max[..., None])
        row_sum = row_sum + jnp.sum(exp_scores, axis=2)
        row_acc = row_acc + jnp.einsum('hqc,hce->hqe', exp_scores.astype(jnp.bfloat16).astype(jnp.float32), v_all[:, key_blk].astype(jnp.float32))
        return (row_sum, row_acc), None

    init_state = (jnp.zeros((NUM_HEADS, glob_rows), jnp.float32), jnp.zeros((NUM_HEADS, glob_rows, HEAD_DIM), jnp.float32))
    totals, ignored = lax.scan(accumulate, init_state, jnp.arange(NUM_BLOCKS))
    glob_out = (totals[1] / totals[0][..., None]).reshape(NUM_HEADS, GLOBAL_BLOCKS, BLOCK_SIZE, HEAD_DIM)
    attended = jnp.concatenate([glob_out.transpose(1, 0, 2, 3), ordinary_out], axis=0)
    attended = attended.transpose(0, 2, 1, 3).reshape(SEQ_LEN, WIDTH).astype(jnp.bfloat16)
    return jnp.dot(attended, w_out.T, preferred_element_type=jnp.float32).astype(jnp.bfloat16)
```

```python
import functools

import jax
import jax.numpy as jnp
from jax import lax
from jax.experimental import pallas as pl
from jax.experimental.pallas import tpu as pltpu
from jax.sharding import PartitionSpec as P

GLOBAL_BLOCKS = 2
HEADS = 12
BLK = 128
LOCAL = 8
SEL = 16
SIDE = 4
FLOWS = 3
ROUNDS = 8
VMEM_LIMIT = 62 * 1024 * 1024
MESH = pl.DeviceIdType.MESH
ORDER = ((0, 1, 2), (1, 2, 0), (2, 0, 1))


def place_of(index):
    return [(index // 2) % SIDE, (index // 8) % SIDE, index // 32], index % 2


def index_of(coords, core):
    return ((coords[2] * SIDE + coords[1]) * SIDE + coords[0]) * 2 + core


def shifted(me, dim, delta, core_delta=0):
    coords, core = place_of(me)
    coords = list(coords)
    coords[dim] = (coords[dim] + delta + SIDE) % SIDE
    return index_of(coords, (core + core_delta) % 2)


def project_kernel(x_ref, wk_ref, wv_ref, wq_ref, out_ref):
    step = pl.program_id(0)
    rows = x_ref.shape[0]
    chunk = 256

    def run(w_ref):
        for r in range(rows // chunk):
            prod = jnp.dot(x_ref[r * chunk:(r + 1) * chunk, :], w_ref[...], preferred_element_type=jnp.float32)
            out_ref[0, r * chunk:(r + 1) * chunk, :] = prod[:, :BLK].astype(jnp.bfloat16)
            out_ref[1, r * chunk:(r + 1) * chunk, :] = prod[:, BLK:].astype(jnp.bfloat16)

    pairs = HEADS // 2

    @pl.when(step < pairs)
    def _():
        run(wk_ref)

    @pl.when((step >= pairs) & (step < 2 * pairs))
    def _():
        run(wv_ref)

    @pl.when(step >= 2 * pairs)
    def _():
        run(wq_ref)


def project_all(x, w_key, w_value, w_query):
    rows, d_model = x.shape
    pairs = HEADS // 2

    def w_spec(first):
        return pl.BlockSpec((d_model, 2 * BLK), lambda j: (0, jnp.clip(j - first, 0, pairs - 1)))

    return pl.pallas_call(
        project_kernel,
        name="project",
        grid=(3 * pairs,),
        in_specs=[pl.BlockSpec((rows, d_model), lambda j: (0, 0)), w_spec(0), w_spec(pairs), w_spec(2 * pairs)],
        out_specs=pl.BlockSpec((2, rows, BLK), lambda j: (j, 0, 0)),
        out_shape=jax.ShapeDtypeStruct((3 * HEADS, rows, BLK), jnp.bfloat16),
        compiler_params=pltpu.CompilerParams(vmem_limit_bytes=40 * 1024 * 1024),
        cost_estimate=pl.CostEstimate(flops=2 * rows * d_model * d_model * 3, bytes_accessed=rows * d_model * 8 + 3 * d_model * d_model * 2, transcendentals=0),
    )(x, w_key, w_value, w_query)


def global_kernel(scale, q_ref, k_ref, v_ref, acc_ref, max_ref, sum_ref):
    scores = lax.dot_general(q_ref[0], k_ref[0], (((1,), (1,)), ((), ())), preferred_element_type=jnp.float32) * scale
    row_max = jnp.max(scores, axis=1, keepdims=True)
    probs = jnp.exp(scores - row_max)
    row_sum = jnp.sum(probs, axis=1, keepdims=True)
    acc_ref[0] = jnp.dot(probs.astype(jnp.bfloat16), v_ref[0], preferred_element_type=jnp.float32)
    max_ref[0] = jnp.broadcast_to(row_max, max_ref.shape[1:])
    sum_ref[0] = jnp.broadcast_to(row_sum, sum_ref.shape[1:])


def global_partial(kvq, glob, scale):
    rows = kvq.shape[1]
    g_rows = glob.shape[1]
    out = jax.ShapeDtypeStruct((HEADS, g_rows, BLK), jnp.float32)
    o_spec = pl.BlockSpec((1, g_rows, BLK), lambda h: (h, 0, 0))
    return pl.pallas_call(
        functools.partial(global_kernel, scale),
        name="global_rows",
        grid=(HEADS,),
        in_specs=[
            pl.BlockSpec((1, g_rows, BLK), lambda h: (h + 2 * HEADS, 0, 0)),
            pl.BlockSpec((1, rows, BLK), lambda h: (h, 0, 0)),
            pl.BlockSpec((1, rows, BLK), lambda h: (h + HEADS, 0, 0)),
        ],
        out_specs=[o_spec, o_spec, o_spec],
        out_shape=[out, out, out],
        compiler_params=pltpu.CompilerParams(vmem_limit_bytes=32 * 1024 * 1024),
        cost_estimate=pl.CostEstimate(flops=4 * HEADS * g_rows * rows * BLK, bytes_accessed=12 * 1024 * 1024, transcendentals=0),
    )(glob, kvq, kvq)


def exchange_kernel(kv_ref, tbl_ref, ag_ref, recv_ref, edge_ref, stage_a, stage_b, send_buf, send_sem, ring_sem, line_sem, load_sem, edge_send, edge_recv):
    me = lax.axis_index("seq")
    n_dev = SIDE ** 3 * 2
    after = lax.rem(me + 1, n_dev)
    before = lax.rem(me + n_dev - 1, n_dev)

    core = lax.rem(me, 2)
    twin = me + 1 - 2 * core
    to_twin = twin - me
    line = {}
    for dim in range(3):
        stride = 2 * SIDE ** dim
        coord = lax.rem(lax.div(me, stride), SIDE)
        for delta in (1, 2, 3):
            line[dim, delta] = me + (lax.rem(coord + delta, SIDE) - coord) * stride
    partners = [twin]
    for dev in line.values():
        partners += [dev, dev + to_twin]
    partners += [after, before]
    barrier = pltpu.get_barrier_semaphore()
    for dev in partners:
        pl.semaphore_signal(barrier, inc=1, device_id={"seq": dev}, device_id_type=MESH)
    pl.semaphore_wait(barrier, len(partners))

    def remote(src, dst, s_sem, r_sem, dev):
        return pltpu.make_async_remote_copy(src_ref=src, dst_ref=dst, send_sem=s_sem, recv_sem=r_sem, device_id={"seq": dev}, device_id_type=MESH)

    edges = [
        remote(kv_ref.at[pl.ds(0, 2 * HEADS), LOCAL - 1], edge_ref.at[0], edge_send.at[0], edge_recv.at[0], after),
        remote(kv_ref.at[pl.ds(0, 2 * HEADS), 0], edge_ref.at[1], edge_send.at[1], edge_recv.at[1], before),
    ]
    for cp in edges:
        cp.start()

    def unit_of(flow, t):
        return lax.rem(t, 2) * HEADS + FLOWS * lax.div(t, 2) + flow

    def ring_copy(stage_id, way, flow, t):
        u = unit_of(flow, t)
        own = kv_ref.at[u]
        got = ag_ref.at[u]
        half = LOCAL // 2
        src, dst = (
            ((own, got.at[3]), (own, got.at[1])),
            ((got.at[3, pl.ds(0, half)], got.at[2, pl.ds(0, half)]), (got.at[1, pl.ds(half, half)], got.at[2, pl.ds(half, half)])),
            ((own, got.at[12]), (own, got.at[4])),
            ((got.at[pl.ds(1, 3)], got.at[pl.ds(13, 3)]), (got.at[pl.ds(1, 3)], got.at[pl.ds(5, 3)])),
            ((got.at[pl.ds(12, 2)], got.at[pl.ds(8, 2)]), (got.at[pl.ds(6, 2)], got.at[pl.ds(10, 2)])),
        )[stage_id][way]
        dim = ORDER[flow][0 if stage_id < 2 else 1]
        dev = line[dim, (1, 3)[way]]
        k = 2 * stage_id + way
        return remote(src, dst, send_sem.at[lax.rem(t, 2), flow, k], ring_sem.at[t, flow, k], dev)

    def line_copy(group, flow, t):
        u = unit_of(flow, t)
        delta, other = group // 2, group % 2
        dst_group = ((SIDE - delta) % SIDE) * 2 + other
        src = send_buf.at[lax.rem(t, 2), flow, pl.ds(group * SIDE * SIDE, SIDE * SIDE)]
        dst = recv_ref.at[u, dst_group]
        if group == 0:
            return pltpu.make_async_copy(src, dst, line_sem.at[t, flow, 0])
        dev = me if delta == 0 else line[ORDER[flow][2], delta]
        dev = dev + to_twin if other else dev
        return remote(src, dst, send_sem.at[lax.rem(t, 2), flow, 10 + group], line_sem.at[t, flow, dst_group], dev)

    def start_ring(stage_ids, t):
        for stage_id in stage_ids:
            for flow in range(FLOWS):
                for way in (0, 1):
                    @pl.when(t >= 2)
                    def _(stage_id=stage_id, flow=flow, way=way):
                        ring_copy(stage_id, way, flow, t - 2).wait_send()
                    ring_copy(stage_id, way, flow, t).start()

    def wait_ring(stage_ids, t):
        for stage_id in stage_ids:
            for flow in range(FLOWS):
                for way in (0, 1):
                    ring_copy(stage_id, way, flow, t).wait_recv()

    def loads(flow, t):
        u = unit_of(flow, t)
        slot = flow % 2
        stage = (stage_a, stage_b)[slot]
        return [
            pltpu.make_async_copy(kv_ref.at[u], stage.at[0], load_sem.at[slot, 0]),
            pltpu.make_async_copy(ag_ref.at[u, pl.ds(1, 15)], stage.at[pl.ds(1, 15)], load_sem.at[slot, 1]),
        ]

    def choose(t):
        for cp in loads(0, t):
            cp.start()
        for flow in range(FLOWS):
            if flow + 1 < FLOWS:
                for cp in loads(flow + 1, t):
                    cp.start()

            @pl.when(t >= 2)
            def _(flow=flow):
                line_copy(0, flow, t - 2).wait()
                for group in range(1, 8):
                    line_copy(group, flow, t - 2).wait_send()

            for cp in loads(flow, t):
                cp.wait()
            base = (FLOWS * lax.div(t, 2) + flow) * (8 * SIDE * SIDE)
            parity = lax.rem(t, 2)

            def pick(n, carry, flow=flow, base=base, parity=parity):
                send_buf[parity, flow, n] = (stage_a, stage_b)[flow % 2][lax.rem(n, SIDE * SIDE), tbl_ref[base + n]]
                return carry

            lax.fori_loop(0, 8 * SIDE * SIDE, pick, 0)
            for group in range(8):
                line_copy(group, flow, t).start()

    def wait_line(t):
        for flow in range(FLOWS):
            for group in range(1, 8):
                line_copy(group, flow, t).wait_recv()

    def step(i, carry):
        def when(lag, fn):
            t = i - lag

            @pl.when((t >= 0) & (t < ROUNDS))
            def _():
                fn(t)

        def first(t):
            start_ring((0, 2), t)

        def second(t):
            wait_ring((0,), t)
            start_ring((1,), t)

        def third(t):
            wait_ring((1,), t)
            start_ring((3,), t)

        def fourth(t):
            wait_ring((2, 3), t)
            start_ring((4,), t)

        def fifth(t):
            wait_ring((4,), t)
            choose(t)

        when(0, first)
        when(1, second)
        when(2, third)
        when(3, fourth)
        when(4, fifth)
        when(5, wait_line)
        return carry

    def drain(t, carry):
        for flow in range(FLOWS):
            for stage_id in range(5):
                for way in (0, 1):
                    ring_copy(stage_id, way, flow, t).wait_send()
            line_copy(0, flow, t).wait()
            for group in range(1, 8):
                line_copy(group, flow, t).wait_send()
        return carry

    lax.fori_loop(0, ROUNDS + 5, step, 0)
    lax.fori_loop(ROUNDS - 2, ROUNDS, drain, 0)
    for cp in edges:
        cp.wait()


def exchange(kvq, table):
    units = 2 * HEADS
    line = SIDE * SIDE
    kv = kvq.reshape(3 * HEADS, LOCAL, BLK, BLK)
    any_spec = pl.BlockSpec(memory_space=pl.ANY)
    ag, recv, edge = pl.pallas_call(
        exchange_kernel,
        name="exchange",
        in_specs=[any_spec, pl.BlockSpec(memory_space=pltpu.SMEM)],
        out_specs=[any_spec, any_spec, any_spec],
        out_shape=[
            jax.ShapeDtypeStruct((units, line, LOCAL, BLK, BLK), jnp.bfloat16),
            jax.ShapeDtypeStruct((units, 8, line, BLK, BLK), jnp.bfloat16),
            jax.ShapeDtypeStruct((2, units, BLK, BLK), jnp.bfloat16),
        ],
        scratch_shapes=[
            pltpu.VMEM((line, LOCAL, BLK, BLK), jnp.bfloat16),
            pltpu.VMEM((line, LOCAL, BLK, BLK), jnp.bfloat16),
            pltpu.VMEM((2, FLOWS, 8 * line, BLK, BLK), jnp.bfloat16),
            pltpu.SemaphoreType.DMA((2, FLOWS, 18)),
            pltpu.SemaphoreType.DMA((ROUNDS, FLOWS, 10)),
            pltpu.SemaphoreType.DMA((ROUNDS, FLOWS, 8)),
            pltpu.SemaphoreType.DMA((2, 2)),
            pltpu.SemaphoreType.DMA((2,)),
            pltpu.SemaphoreType.DMA((2,)),
        ],
        compiler_params=pltpu.CompilerParams(collective_id=0, has_side_effects=True, vmem_limit_bytes=VMEM_LIMIT),
        cost_estimate=pl.CostEstimate(flops=10 ** 12, bytes_accessed=4 * 10 ** 8, transcendentals=0),
    )(kv, table)
    del ag
    return recv, edge


def attend_kernel(scale, pos_ref, bias_ref, q_ref, k_ref, v_ref, ek_ref, ev_ref, gk_ref, gv_ref, rk_ref, rv_ref, out_ref, scores):
    head = pl.program_id(0)
    n_keys = GLOBAL_BLOCKS + 3 + SEL

    def window(local_ref, edge_ref, i, off):
        if off == 0:
            return local_ref[0, i]
        if off < 0:
            return jnp.where(i == 0, edge_ref[0, 0], local_ref[0, jnp.maximum(i - 1, 0)])
        return jnp.where(i == LOCAL - 1, edge_ref[1, 0], local_ref[0, jnp.minimum(i + 1, LOCAL - 1)])

    def block_of(j, i, g_ref, local_ref, edge_ref, r_ref):
        if j < GLOBAL_BLOCKS:
            return g_ref[0, j]
        if j < GLOBAL_BLOCKS + 3:
            return window(local_ref, edge_ref, i, j - GLOBAL_BLOCKS - 1)
        return r_ref[0, pos_ref[(head * LOCAL + i) * SEL + j - GLOBAL_BLOCKS - 3]]

    def row_block(i, carry):
        q = q_ref[0, i]
        base = (head * LOCAL + i) * n_keys
        top = None
        for j in range(n_keys):
            k_blk = block_of(j, i, gk_ref, k_ref, ek_ref, rk_ref)
            s = lax.dot_general(q, k_blk, (((1,), (1,)), ((), ())), preferred_element_type=jnp.float32) * scale + bias_ref[base + j]
            scores[j] = s
            top = s if top is None else jnp.maximum(top, s)
        row_max = jnp.max(top, axis=1, keepdims=True)
        total = jnp.zeros((BLK, BLK), jnp.float32)
        acc = jnp.zeros((BLK, BLK), jnp.float32)
        for j in range(n_keys):
            p = jnp.exp(scores[j] - row_max)
            total = total + p
            v_blk = block_of(j, i, gv_ref, v_ref, ev_ref, rv_ref)
            acc = acc + jnp.dot(p.astype(jnp.bfloat16), v_blk, preferred_element_type=jnp.float32)
        out = acc / jnp.sum(total, axis=1, keepdims=True)
        out_ref[pl.ds(pl.multiple_of(i * BLK, BLK), BLK), :] = out.astype(jnp.bfloat16)
        return carry

    lax.fori_loop(0, LOCAL, row_block, 0)


def attend(kvq, glob, recv, edge, pos, bias, scale):
    units = 2 * HEADS
    kvq4 = kvq.reshape(3 * HEADS, LOCAL, BLK, BLK)
    glob4 = glob.reshape(3 * HEADS, GLOBAL_BLOCKS, BLK, BLK)
    recv4 = recv.reshape(units, 8 * SIDE * SIDE, BLK, BLK)

    def spec(n, first):
        return pl.BlockSpec((1, n, BLK, BLK), lambda h, *_: (h + first, 0, 0, 0))

    def e_spec(first):
        return pl.BlockSpec((2, 1, BLK, BLK), lambda h, *_: (0, h + first, 0, 0))

    n_keys = GLOBAL_BLOCKS + 3 + SEL
    return pl.pallas_call(
        functools.partial(attend_kernel, scale),
        name="attend",
        grid_spec=pltpu.PrefetchScalarGridSpec(
            num_scalar_prefetch=2,
            grid=(HEADS,),
            in_specs=[
                spec(LOCAL, 2 * HEADS), spec(LOCAL, 0), spec(LOCAL, HEADS), e_spec(0), e_spec(HEADS),
                spec(GLOBAL_BLOCKS, 0), spec(GLOBAL_BLOCKS, HEADS), spec(8 * SIDE * SIDE, 0), spec(8 * SIDE * SIDE, HEADS),
            ],
            out_specs=pl.BlockSpec((LOCAL * BLK, BLK), lambda h, *_: (0, h)),
            scratch_shapes=[pltpu.VMEM((n_keys, BLK, BLK), jnp.float32)],
        ),
        out_shape=jax.ShapeDtypeStruct((LOCAL * BLK, HEADS * BLK), jnp.bfloat16),
        compiler_params=pltpu.CompilerParams(vmem_limit_bytes=48 * 1024 * 1024),
        cost_estimate=pl.CostEstimate(flops=4 * HEADS * LOCAL * n_keys * BLK ** 3, bytes_accessed=11 * 10 ** 7, transcendentals=0),
    )(pos, bias, kvq4, kvq4, kvq4, edge, edge, glob4, glob4, recv4, recv4)


def key_mask(selected, row_ids, n_blocks):
    n_heads, n_local, n_sel = selected.shape
    n_glob = GLOBAL_BLOCKS
    window_raw = row_ids[:, None] + jnp.arange(-1, 2)
    window_ok = (window_raw >= n_glob) & (window_raw < n_blocks)
    earlier = jnp.arange(n_sel)[None, :] < jnp.arange(n_sel)[:, None]
    repeat = jnp.any((selected[:, :, :, None] == selected[:, :, None, :]) & earlier, axis=3)
    sel_ok = (selected >= n_glob) & (jnp.abs(selected - row_ids[:, None]) > 1) & jnp.logical_not(repeat)
    return jnp.concatenate([jnp.full((n_heads, n_local, n_glob), True), jnp.broadcast_to(window_ok, (n_heads, n_local, 3)), sel_ok], axis=2)


def places(selected, me):
    owner, local_id = selected // LOCAL, selected % LOCAL
    coords, core = place_of(me)
    o_coords, o_core = place_of(owner)
    rel = [(o - m) % SIDE for o, m in zip(o_coords, coords)]
    rel_core = (o_core - core) % 2
    flow = (jnp.arange(HEADS) % FLOWS)[:, None, None]

    def along(which):
        return sum(jnp.where(flow == f, rel[ORDER[f][which]], 0) for f in range(FLOWS))

    pos = ((along(2) * 2 + rel_core) * SIDE + along(1)) * SIDE + along(0)
    return pos, local_id


def request_table(pos, local_id, me):
    n_pos = 8 * SIDE * SIDE
    flat_pos, flat_id = pos.reshape(HEADS, -1), local_id.reshape(HEADS, -1)
    hit = flat_pos[:, :, None] == jnp.arange(n_pos)
    wanted = jnp.max(jnp.where(hit, flat_id[:, :, None], 0), axis=1)
    every = lax.all_gather(wanted, 'seq')
    heads = jnp.arange(HEADS)[:, None]
    group = jnp.arange(8)[None, :]
    delta, other = group // 2, group % 2
    dev = sum(jnp.where(heads % FLOWS == f, shifted(me, ORDER[f][2], delta, other), 0) for f in range(FLOWS))
    theirs = ((SIDE - delta) % SIDE) * 2 + other
    every = every.reshape(-1, HEADS, 8, SIDE * SIDE)
    return every[dev, heads, theirs].reshape(-1)


def solution(mesh):
    n_shards = mesh.shape['seq']

    def per_device(tokens, w_query, w_key, w_value, w_out, selected):
        n_glob = GLOBAL_BLOCKS
        g_rows = n_glob * BLK
        n_blocks = LOCAL * n_shards
        scale = BLK ** -0.5
        me = lax.axis_index('seq')
        is_first = me == 0
        row_ids = me * LOCAL + jnp.arange(LOCAL)

        glob_x = lax.psum(jnp.where(is_first, tokens[:g_rows], 0), 'seq')
        pos, local_id = places(selected, me)
        table = request_table(pos, local_id, me)
        key_ok = key_mask(selected, row_ids, n_blocks)
        bias = jnp.where(key_ok, 0.0, -jnp.inf).astype(jnp.float32).reshape(-1)

        kvq = project_all(tokens, w_key, w_value, w_query)
        glob = project_all(glob_x, w_key, w_value, w_query)

        part_acc, part_max, part_sum = global_partial(kvq, glob, scale)
        part_max, part_sum = part_max[:, :, :1], part_sum[:, :, :1]
        top = lax.pmax(part_max[:, :, 0], 'seq')[:, :, None]
        shrink = jnp.exp(part_max - top)
        row_sum = lax.psum(part_sum * shrink, 'seq')
        row_acc = lax.psum(part_acc * shrink, 'seq')

        recv, edge = exchange(kvq, table)
        attended = attend(kvq, glob, recv, edge, pos.reshape(-1), bias, scale)

        glob_out = (row_acc / row_sum).astype(jnp.bfloat16)
        glob_out = glob_out.transpose(1, 0, 2).reshape(g_rows, HEADS * BLK)
        head_rows = jnp.where(is_first, glob_out, attended[:g_rows])
        attended = attended.at[:g_rows].set(head_rows)
        mixed = lax.dot_general(attended, w_out, (((1,), (1,)), ((), ())), preferred_element_type=jnp.float32)
        return mixed.astype(jnp.bfloat16)

    row_spec = P(('batch', 'seq'), None)
    full_spec = P()
    sel_spec = P(None, ('batch', 'seq'), None)
    return jax.shard_map(per_device, mesh=mesh, in_specs=(row_spec, full_spec, full_spec, full_spec, full_spec, sel_spec), out_specs=row_spec, check_vma=False)
```
